16 devices in a mesh: vp: 2 (over z), dp: 8 (over y, x, core).
Axes of the slice: x: 2, y: 2, z: 2, core: 2. Of those that a mesh axis runs over, the one named last changes fastest.
Arguments:
- h_last: bfloat16 [4096, 49, 768], P('dp')
- ln_gamma: float32 [768], replicated
- ln_beta: float32 [768], replicated
- w_cls: bfloat16 [768, 22016], P(None, 'vp')
- b_cls: float32 [22016], P('vp')
- targets: float32 [4096, 22016], P('dp', 'vp')
Outputs:
- output 1: float32 [], replicated
- output 2: float32 [768, 22016], P(None, 'vp')
- output 3: float32 [22016], P('vp')
- output 4: bfloat16 [4096, 49, 768], P('dp')
All inputs are finite; a program needn't handle non-finite values.
Results may differ from the reference program's by a relative error of at most 0.001.
Values sent between devices are 32-bit elements.
A program may use at most 1 GiB of HBM per device.

```python
import jax
import jax.numpy as jnp
from jax import lax

IMG_DEV = 512
DP_SIZE = 8
TOKENS = 49
WIDTH = 768
CLASSES = 21841
CLASSES_PAD = 22016
N_GLOB = IMG_DEV * DP_SIZE
LN_EPS = 1e-5


def pool_norm(h_blk, ln_gamma, ln_beta):
    h_wide = h_blk.astype(jnp.float32)
    tok_mean = h_wide.mean(axis=-1, keepdims=True)
    centered = h_wide - tok_mean
    tok_var = (centered * centered).mean(axis=-1, keepdims=True)
    normed = centered * lax.rsqrt(tok_var + LN_EPS)
    return (normed * ln_gamma + ln_beta).mean(axis=1)


def setup_inputs(seed: int = 0) -> dict:
    root_key = jax.random.key(seed)
    sub_keys = jax.random.split(root_key, 8)
    img_base = jax.random.normal(sub_keys[0], (N_GLOB, 1, WIDTH), jnp.float32)
    tok_noise = jax.random.normal(sub_keys[1], (N_GLOB, TOKENS, WIDTH), jnp.float32)
    h_last = (img_base + 0.5 * tok_noise).astype(jnp.bfloat16)
    ln_gamma = 2.0 + 0.5 * jax.random.normal(sub_keys[2], (WIDTH,), jnp.float32)
    ln_beta = 0.5 * jax.random.normal(sub_keys[3], (WIDTH,), jnp.float32)
    w_cls = (jax.random.normal(sub_keys[4], (WIDTH, CLASSES_PAD), jnp.float32) * WIDTH ** -0.5).astype(jnp.bfloat16)
    b_cls = jax.random.normal(sub_keys[5], (CLASSES_PAD,), jnp.float32)
    classes = jax.random.randint(sub_keys[6], (N_GLOB, 2), 0, CLASSES)
    mix_lam = jax.random.uniform(sub_keys[7], (N_GLOB, 1), jnp.float32)
    col_idx = jnp.arange(CLASSES_PAD)
    first_hit = (col_idx[None, :] == classes[:, 0:1]).astype(jnp.float32)
    second_hit = (col_idx[None, :] == classes[:, 1:2]).astype(jnp.float32)
    smooth = jnp.where(col_idx < CLASSES, 0.1 / CLASSES, 0.0)
    targets = 0.9 * (mix_lam * first_hit + (1.0 - mix_lam) * second_hit) + smooth[None, :]
    return {"h_last": h_last, "ln_gamma": ln_gamma, "ln_beta": ln_beta, "w_cls": w_cls, "b_cls": b_cls, "targets": targets}


def reference(h_last, ln_gamma, ln_beta, w_cls, b_cls, targets):
    in_range = jnp.arange(CLASSES_PAD) < CLASSES
    h_blocks = h_last.reshape(DP_SIZE, IMG_DEV, TOKENS, WIDTH)
    t_blocks = targets.reshape(DP_SIZE, IMG_DEV, CLASSES_PAD)

    def block_step(acc_state, block_in):
        dw_acc, db_acc, loss_acc = acc_state
        h_blk, t_blk = block_in
        pooled, pool_vjp = jax.vjp(lambda h_in: pool_norm(h_in, ln_gamma, ln_beta), h_blk)
        pooled_bf = pooled.astype(jnp.bfloat16)
        logits = jnp.dot(pooled_bf, w_cls, preferred_element_type=jnp.float32) + b_cls
        masked = jnp.where(in_range, logits, -jnp.inf)
        log_norm = jax.nn.logsumexp(masked, axis=1)
        t_sum = t_blk.sum(axis=1)
        t_dot = (t_blk * jnp.where(in_range, logits, 0.0)).sum(axis=1)
        soft_prob = jnp.exp(masked - log_norm[:, None])
        dlogits = (soft_prob * t_sum[:, None] - t_blk) / N_GLOB
        dlog_bf = dlogits.astype(jnp.bfloat16)
        dw_blk = jnp.dot(pooled_bf.T, dlog_bf, preferred_element_type=jnp.float32)
        d_pooled = jnp.dot(dlog_bf, w_cls.T, preferred_element_type=jnp.float32)
        dh_blk = pool_vjp(d_pooled)[0]
        loss_blk = (log_norm * t_sum - t_dot).sum()
        return (dw_acc + dw_blk, db_acc + dlogits.sum(axis=0), loss_acc + loss_blk), dh_blk

    carry_init = (jnp.zeros((WIDTH, CLASSES_PAD), jnp.float32), jnp.zeros((CLASSES_PAD,), jnp.float32), jnp.zeros((), jnp.float32))
    (dw_cls, db_cls, loss_sum), dh_blocks = lax.scan(block_step, carry_init, (h_blocks, t_blocks))
    return loss_sum / N_GLOB, dw_cls, db_cls, dh_blocks.reshape(N_GLOB, TOKENS, WIDTH)
```

```python
import functools

import jax
import jax.numpy as jnp
from jax import lax
from jax.experimental import pallas as pl
from jax.experimental.pallas import tpu as pltpu
from jax.sharding import PartitionSpec as P

NUM_CLASSES = 21841
LN_EPS = 1e-5
CHUNKS = (5, 5, 12, 12, 13, 13, 13, 13)
LANES = 128


def ln_fwd_kernel(h_ref, gamma_ref, beta_ref, u_ref, *, tokens, width):
    def one(tok, acc):
        x = h_ref[tok].astype(jnp.float32)
        c = x - jnp.sum(x, axis=-1, keepdims=True) * (1.0 / width)
        var = jnp.sum(c * c, axis=-1, keepdims=True) * (1.0 / width)
        return acc + c * lax.rsqrt(var + LN_EPS)

    acc = lax.fori_loop(0, tokens, one, jnp.zeros(u_ref.shape, jnp.float32), unroll=7)
    u_ref[...] = acc * (1.0 / tokens) * gamma_ref[...] + beta_ref[...]


def ln_fwd(ht, gamma, beta, rows=16):
    tokens, images, width = ht.shape
    return pl.pallas_call(
        functools.partial(ln_fwd_kernel, tokens=tokens, width=width),
        grid=(images // rows,),
        in_specs=[
            pl.BlockSpec((tokens, rows, width), lambda i: (0, i, 0)),
            pl.BlockSpec((1, width), lambda i: (0, 0)),
            pl.BlockSpec((1, width), lambda i: (0, 0)),
        ],
        out_specs=pl.BlockSpec((rows, width), lambda i: (i, 0)),
        out_shape=jax.ShapeDtypeStruct((images, width), jnp.float32),
        compiler_params=pltpu.CompilerParams(dimension_semantics=("arbitrary",)),
        cost_estimate=pl.CostEstimate(flops=30_000_000_000, bytes_accessed=ht.size * 2, transcendentals=0),
        name="ln_fwd",
    )(ht, gamma.reshape(1, width), beta.reshape(1, width))


def ln_bwd_kernel(h_ref, du_ref, gamma_ref, dh_ref, *, tokens, width):
    dy = du_ref[...] * (gamma_ref[...] * (1.0 / tokens))
    dyc = dy - jnp.sum(dy, axis=-1, keepdims=True) * (1.0 / width)

    def one(tok, carry):
        x = h_ref[tok].astype(jnp.float32)
        c = x - jnp.sum(x, axis=-1, keepdims=True) * (1.0 / width)
        var = jnp.sum(c * c, axis=-1, keepdims=True) * (1.0 / width)
        r = lax.rsqrt(var + LN_EPS)
        q = jnp.sum(dy * c, axis=-1, keepdims=True) * (1.0 / width)
        dh_ref[tok] = (dyc * r - c * (r * r * r * q)).astype(dh_ref.dtype)
        return carry

    lax.fori_loop(0, tokens, one, 0, unroll=7)


def ln_bwd(ht, du, gamma, rows=16):
    tokens, images, width = ht.shape
    return pl.pallas_call(
        functools.partial(ln_bwd_kernel, tokens=tokens, width=width),
        grid=(images // rows,),
        in_specs=[
            pl.BlockSpec((tokens, rows, width), lambda i: (0, i, 0)),
            pl.BlockSpec((rows, width), lambda i: (i, 0)),
            pl.BlockSpec((1, width), lambda i: (0, 0)),
        ],
        out_specs=pl.BlockSpec((tokens, rows, width), lambda i: (0, i, 0)),
        out_shape=jax.ShapeDtypeStruct(ht.shape, ht.dtype),
        compiler_params=pltpu.CompilerParams(dimension_semantics=("arbitrary",)),
        cost_estimate=pl.CostEstimate(flops=40_000_000_000, bytes_accessed=ht.size * 4, transcendentals=0),
        name="ln_bwd",
    )(ht, du, gamma.reshape(1, width))


def place_kernel(*refs, col, first, order):
    pieces = refs[:8]
    out_ref, buf, load_sem, store_sem = refs[-4:]
    rows, cols = buf.shape[1:]
    core = lax.rem(lax.axis_index("dp"), 2)
    x = lax.rem(lax.axis_index("dp") // 2, 2)
    y = lax.axis_index("dp") // 4
    bits = (core, x, y) if order == 0 else (core, y, x)

    def load(r):
        return pltpu.make_async_copy(pieces[r], buf.at[r], load_sem.at[r])

    def store(r):
        block = 0
        for k, bit in enumerate(bits):
            want = (r >> (2 - k)) & 1
            block = block * 2 + (bit if want == 0 else 1 - bit)
        row = pl.multiple_of(block * rows, rows)
        return pltpu.make_async_copy(buf.at[r], out_ref.at[pl.ds(row, rows), pl.ds(col, cols)], store_sem.at[r])

    for r in range(8):
        load(r).start()
    for r in range(8):
        load(r).wait()
        store(r).start()
    for r in range(8):
        store(r).wait()


def place(out, pieces, col, order, shape):
    rows, cols = pieces[0].shape
    hbm = pl.BlockSpec(memory_space=pl.ANY)
    args = list(pieces) + ([] if out is None else [out])
    return pl.pallas_call(
        functools.partial(place_kernel, col=col, first=out is None, order=order),
        in_specs=[hbm] * len(args),
        out_specs=hbm,
        out_shape=jax.ShapeDtypeStruct(shape, jnp.float32),
        scratch_shapes=[
            pltpu.VMEM((8, rows, cols), jnp.float32),
            pltpu.SemaphoreType.DMA((8,)),
            pltpu.SemaphoreType.DMA((8,)),
        ],
        input_output_aliases={} if out is None else {8: 0},
        cost_estimate=pl.CostEstimate(flops=1_000_000_000, bytes_accessed=16 * rows * cols * 4, transcendentals=0),
        name="place",
    )(*args)


def solution(mesh):
    dp_size = mesh.shape["dp"]

    def swap(val, axis):
        if axis == "vp":
            return lax.ppermute(val, "vp", [(0, 1), (1, 0)])
        flip = {"core": 1, "x": 2, "y": 4}[axis]
        return lax.ppermute(val, "dp", [(i, i ^ flip) for i in range(dp_size)])

    def local_step(h_loc, gamma, beta, w_loc, b_loc, t_loc):
        images, tokens, width = h_loc.shape
        n_glob = images * dp_size
        cls_local = w_loc.shape[1]
        vp = lax.axis_index("vp")
        dp = lax.axis_index("dp")
        core, x, y = dp % 2, (dp // 2) % 2, dp // 4
        ht = h_loc.transpose(1, 0, 2)
        pooled_bf = ln_fwd(ht, gamma, beta).astype(jnp.bfloat16)
        in_range = vp * cls_local + jnp.arange(cls_local) < NUM_CLASSES
        logits = jnp.dot(pooled_bf, w_loc, preferred_element_type=jnp.float32) + b_loc
        masked = jnp.where(in_range, logits, -jnp.inf)
        top = masked.max(axis=1)
        expo = jnp.exp(masked - top[:, None])
        t_dot = (t_loc * jnp.where(in_range, logits, 0.0)).sum(axis=1)
        mine = jnp.stack([top, expo.sum(axis=1), t_loc.sum(axis=1), t_dot])
        theirs = swap(mine, "vp")
        lo, hi = jnp.where(vp == 0, mine, theirs), jnp.where(vp == 0, theirs, mine)
        row_max = jnp.maximum(lo[0], hi[0])
        norm = lo[1] * jnp.exp(lo[0] - row_max) + hi[1] * jnp.exp(hi[0] - row_max)
        t_sum = lo[2] + hi[2]
        loss_part = ((row_max + jnp.log(norm)) * t_sum - (lo[3] + hi[3])).sum()
        scale = t_sum / norm

        half_a = jnp.stack([core * 4 + x * 2 + y, core * 4 + y * 2 + x])
        blocks = pooled_bf.T.reshape(8, width // 8, images)
        u_rel = [jnp.take(blocks, jnp.arange(8) ^ half_a[o], axis=0).reshape(width, images) for o in range(2)]

        rows = width // 8
        dlogits = (jnp.exp(masked - row_max[:, None]) * scale[:, None] - t_loc) / n_glob
        dlog_bf = dlogits.astype(jnp.bfloat16)
        db_part = dlogits.sum(axis=0)
        d_part = lax.dot_general(dlog_bf, w_loc, (((1,), (1,)), ((), ())), preferred_element_type=jnp.float32)
        d_pooled = d_part + swap(d_part, "vp")
        dh_loc = ln_bwd(ht, d_pooled, gamma).transpose(1, 0, 2)

        out, col = None, 0
        for j, wide in enumerate(CHUNKS):
            order = j % 2
            first, second = ("x", "y") if order == 0 else ("y", "x")
            cols = wide * LANES
            g = dlog_bf[:, col:col + cols]
            send0 = jnp.dot(u_rel[order][4 * rows:], g, preferred_element_type=jnp.float32)
            keep0 = jnp.dot(u_rel[order][:4 * rows], g, preferred_element_type=jnp.float32)
            got0 = swap(send0, "core")
            send1 = keep0[2 * rows:] + got0[2 * rows:]
            got1 = swap(send1, first)
            send2 = keep0[rows:2 * rows] + got0[rows:2 * rows] + got1[rows:]
            got2 = swap(send2, second)
            f0 = keep0[:rows] + got0[:rows] + got1[:rows] + got2
            f1 = swap(f0, second)
            f2 = swap(f0, first)
            f3 = swap(f1, first)
            pieces = [f0, f1, f2, f3]
            pieces += [swap(f, "core") for f in pieces]
            out = place(out, pieces, col, order, (width, cls_local))
            col += cols

        tail = jnp.concatenate([db_part, jnp.full((LANES,), loss_part)])
        for axis in ("core", "x", "y"):
            tail = tail + swap(tail, axis)
        return tail[cls_local] / n_glob, out, tail[:cls_local], dh_loc

    return jax.shard_map(local_step, mesh=mesh, in_specs=(P("dp", None, None), P(), P(), P(None, "vp"), P("vp"), P("dp", "vp")), out_specs=(P(), P(None, "vp"), P("vp"), P("dp", None, None)), check_vma=False)
```
